32 devices in a mesh: pix: 8 (over z, y), lat: 4 (over x, core).
Axes of the slice: x: 2, y: 2, z: 4, core: 2. Of those that a mesh axis runs over, the one named last changes fastest.
Arguments:
- latents: float32 [2048, 512], P('lat'), as said below
- pixel_keys: float32 [4096, 512], P('pix'), as said below
- pixel_values: float32 [4096, 512], P('pix'), may hold values from -6 to 6
- norm_gain: float32 [512], replicated, may hold values from 0.1 to 1.9
- w_key: float32 [512, 512], replicated, may hold values from -0.25 to 0.25
- w_value: float32 [512, 512], replicated, may hold values from -0.25 to 0.25
- pixel_queries: float32 [4096, 512], P('pix'), as said below
Outputs:
- latent_state: float32 [2048, 512], P('lat')
- pixel_out: float32 [4096, 512], P('pix')
The draws below stay inside these ranges and needn't reach their ends.
Inputs may be any that keep to these rules, and one draw needn't show every extreme that they name: Real-valued latents. `pixel_keys`: Real-valued keys. `pixel_queries`: Real-valued queries.
All inputs are finite; a program needn't handle non-finite values.
Results may differ from the reference program's by a relative error of at most 0.0003.
Values sent between devices are 32-bit elements; how exact they have to be, the bound alone decides.
No kernel may reach another device: no remote copies, remote signals or barrier semaphores. Data moves between devices by JAX's collectives and lax.ppermute only.
A program may use at most 64 MiB of HBM per device.

```python
import jax
import jax.numpy as jnp
from jax import lax

D = 512
L = 2048
PIXELS = 4096


def keys_table(key):
    table = 4.0 * jax.random.normal(jax.random.fold_in(key, 11), (PIXELS, D), jnp.float32)
    return table


def draw_pixel_keys(key, part):
    return keys_table(key)


def draw_latents(key, part):
    base = jax.random.normal(jax.random.fold_in(key, 23), (L, D), jnp.float32)
    return base


def draw_pixel_queries(key, part):
    base = jax.random.normal(jax.random.fold_in(key, 31), (PIXELS, D), jnp.float32)
    return base


def level_of(key, shape, cuts, smallest, high):
    level, own = 1.0, jax.random.fold_in(key, 6)
    for position, shards_of in cuts:
        draws = jnp.exp(jax.random.uniform(jax.random.fold_in(own, position), (shards_of,), jnp.float32, smallest / len(cuts), high / len(cuts)))
        level = level * jnp.repeat(draws, shape[position] // shards_of).reshape([-1 if axis == position else 1 for axis in range(len(shape))])
    return level


def scatter_about(rng, dims, scale, bound, split=(), held_as=jnp.bfloat16):
    factor_of = level_of(rng, dims, split, -0.22, 0.18) if split else 1.0
    values = jax.random.normal(rng, dims, jnp.float32) * scale * factor_of
    return jnp.minimum(jnp.maximum(values, -bound), bound).astype(held_as)


def setup_inputs(seed: int = 0) -> dict:
    streams_of = jax.random.split(jax.random.key(seed), 8)
    return {
        "latents": draw_latents(jax.random.fold_in(streams_of[7], 71), 0),
        "pixel_keys": draw_pixel_keys(jax.random.fold_in(streams_of[7], 71), 0),
        "pixel_values": scatter_about(streams_of[2], (PIXELS, D), 1.0, 6.0, ((0, 8),), jnp.float32),
        "norm_gain": jnp.clip(1.0 + 0.18 * jax.random.normal(streams_of[3], (D,), jnp.float32), 0.1, 1.9),
        "w_key": scatter_about(streams_of[4], (D, D), D ** -0.5, 0.25, (), jnp.float32),
        "w_value": scatter_about(streams_of[5], (D, D), D ** -0.5, 0.25, (), jnp.float32),
        "pixel_queries": draw_pixel_queries(jax.random.fold_in(streams_of[7], 71), 0),
    }


def attend(queries, keys, values):
    scores = jnp.dot(queries, keys.T, precision=lax.Precision.HIGHEST) / jnp.sqrt(jnp.float32(D))
    top = lax.optimization_barrier(jnp.max(scores, axis=1, keepdims=True))
    weights = jnp.exp(scores - top)
    total = lax.optimization_barrier(jnp.sum(weights, axis=1, keepdims=True))
    return jnp.dot(weights, values, precision=lax.Precision.HIGHEST) / total

def reference(latents, pixel_keys, pixel_values, norm_gain, w_key, w_value, pixel_queries):
    block = 128
    blocks = latents.reshape(L // block, block, D)
    read = lax.map(lambda rows: attend(rows, pixel_keys, pixel_values), blocks).reshape(L, D)
    latent_state = latents + read
    normed = latent_state / jnp.sqrt(lax.optimization_barrier(jnp.mean(latent_state * latent_state, axis=1, keepdims=True)) + 1e-06) * norm_gain
    latent_keys = jnp.dot(normed, w_key, precision=lax.Precision.HIGHEST)
    latent_values = jnp.dot(normed, w_value, precision=lax.Precision.HIGHEST)
    pblock = min(1024, PIXELS)
    pblocks = pixel_queries.reshape(PIXELS // pblock, pblock, D)
    pixel_out = lax.map(lambda rows: attend(rows, latent_keys, latent_values), pblocks).reshape(PIXELS, D)
    return (latent_state, pixel_out)
```

```python
import functools

import jax
import jax.numpy as jnp
from jax import lax
from jax.experimental import pallas as pl
from jax.experimental.pallas import tpu as pltpu
from jax.sharding import PartitionSpec as P

STAT = 8
PARAMS = pltpu.CompilerParams(vmem_limit_bytes=24 * 1024 * 1024)
VMEM = pl.BlockSpec(memory_space=pltpu.VMEM)
SMEM = pl.BlockSpec(memory_space=pltpu.SMEM)


def split(x):
    hi = x.astype(jnp.bfloat16)
    lo = (x - hi.astype(jnp.float32)).astype(jnp.bfloat16)
    return hi, lo


def dot3(a, b, dims):
    (ah, al), (bh, bl) = a, b
    dot = functools.partial(
        lax.dot_general, dimension_numbers=(dims, ((), ())), preferred_element_type=jnp.float32
    )
    return dot(ah, bh) + (dot(ah, bl) + dot(al, bh))


NT = ((1,), (1,))
NN = ((1,), (0,))


def call(body, outs, specs, scratch=(), name=None):
    return pl.pallas_call(
        body,
        out_shape=tuple(jax.ShapeDtypeStruct(s, jnp.float32) for s in outs),
        in_specs=list(specs),
        out_specs=tuple(VMEM for _ in outs),
        scratch_shapes=list(scratch),
        compiler_params=PARAMS,
        name=name,
    )


def pack_stats(top, total):
    rows = top.shape[0]
    lane = lax.broadcasted_iota(jnp.int32, (rows, 128), 1)
    wide = jnp.where(lane == 0, top, jnp.where(lane == 1, total, 0.0))
    return wide.T[:STAT]


def unpack_stats(tile):
    rows = tile.shape[1]
    wide = jnp.concatenate([tile] * (128 // STAT), axis=0).T
    return wide[:, 0:1], wide[:, 1:2]


def attend(scores):
    top = jnp.max(scores, axis=1, keepdims=True)
    weights = jnp.exp(scores - top)
    return top, weights, jnp.sum(weights, axis=1, keepdims=True)


def merge(parts):
    top = functools.reduce(jnp.maximum, [p[0] for p in parts])
    total = weighted = None
    for t, s, w in parts:
        scale = jnp.exp(t - top)
        total = s * scale if total is None else total + s * scale
        weighted = w * scale if weighted is None else weighted + w * scale
    return top, total, weighted


def load_packed(ref, rows):
    top, total = unpack_stats(ref[rows:rows + STAT, :rows])
    return top, total, ref[:rows]


def store_packed(ref, rows, part):
    top, total, weighted = part
    ref[:rows] = weighted
    ref[rows:rows + STAT, :rows] = pack_stats(top, total)
    if rows < ref.shape[1]:
        ref[rows:rows + STAT, rows:] = jnp.zeros((STAT, ref.shape[1] - rows), jnp.float32)


def partial_kernel(rank, queries, keys, values, *rest, blocks, scale):
    outs, (acc, stats) = rest[:blocks], rest[blocks:]
    scores = dot3(split(queries[...] * scale), split(keys[...]), NT)
    top, weights, total = attend(scores)
    acc[...] = dot3(split(weights), split(values[...]), NN)
    lane = lax.broadcasted_iota(jnp.int32, stats.shape, 1)
    stats[...] = jnp.where(lane == 0, top, total)
    rows = queries.shape[0] // blocks
    for k in range(blocks):
        at = pl.multiple_of((rank[0] ^ k) * rows, rows)
        block = pl.ds(at, rows)
        st = stats[block, :]
        store_packed(outs[k], rows, (st[:, 0:1], st[:, 1:2], acc[block, :]))


def merge_kernel(*refs, rows):
    store_packed(refs[-1], rows, merge([load_packed(r, rows) for r in refs[:-1]]))


def state_kernel(rank, latents, *refs, rows):
    _, total, weighted = merge([load_packed(r, rows) for r in refs[:-1]])
    at = pl.multiple_of(rank[0] * rows, rows)
    refs[-1][...] = latents[pl.ds(at, rows), :] + weighted / total


def query_kernel(queries, w_key, out, *, scale):
    out[...] = dot3(split(queries[...] * scale), split(w_key[...]), NT)


def read_kernel(ranks, queries, gain, *refs, blocks, halves):
    states, state_out, outs = refs[:blocks], refs[blocks], refs[blocks + 1:blocks + 1 + halves]
    acc, stats = refs[blocks + 1 + halves:]
    rows = states[0].shape[0]
    for k in range(blocks):
        at = pl.multiple_of((ranks[0] ^ k) * rows, rows)
        state_out[pl.ds(at, rows), :] = states[k][...]
    state = state_out[...]
    normed = state / jnp.sqrt(jnp.mean(state * state, axis=1, keepdims=True) + 1e-06) * gain[...]
    parts = split(normed)
    scores = dot3(split(queries[...]), parts, NT)
    top, weights, total = attend(scores)
    acc[...] = dot3(split(weights), parts, NN)
    lane = lax.broadcasted_iota(jnp.int32, stats.shape, 1)
    stats[...] = jnp.where(lane == 0, top, total)
    rows = queries.shape[0] // halves
    for k in range(halves):
        at = pl.multiple_of((ranks[1] ^ k) * rows, rows)
        block = pl.ds(at, rows)
        st = stats[block, :]
        store_packed(outs[k], rows, (st[:, 0:1], st[:, 1:2], acc[block, :]))


def mean_kernel(*refs, rows):
    _, total, weighted = merge([load_packed(r, rows) for r in refs[:-1]])
    refs[-1][...] = weighted / total


def out_kernel(rank, w_value, *refs, halves):
    parts, out = refs[:halves], refs[halves]
    rows = parts[0].shape[0]
    weight = split(w_value[...])
    for k in range(halves):
        at = pl.multiple_of((rank[0] ^ k) * rows, rows)
        out[pl.ds(at, rows), :] = dot3(split(parts[k][...]), weight, NN)


def swap(value, axis, n, mask):
    return lax.ppermute(value, axis, [(i, i ^ mask) for i in range(n)])


def shards(latents, pixel_keys, pixel_values, norm_gain, w_key, w_value, pixel_queries, *, npix, nlat):
    depth = latents.shape[1]
    scale = depth ** -0.5
    pix, lat = lax.axis_index("pix"), lax.axis_index("lat")
    group = min(4, npix)
    rank = pix & (group - 1)
    outer = []
    step = group
    while step < npix:
        outer.append(step)
        step *= 2
    if outer and group == 4:
        outer[0] = 6
        rank = rank ^ jnp.where(pix & 4, 2, 0)
    rank = rank.reshape(1)
    rows = latents.shape[0] // group
    packed = (rows + STAT, depth)

    partials = call(
        functools.partial(partial_kernel, blocks=group, scale=scale),
        [packed] * group,
        [SMEM, VMEM, VMEM, VMEM],
        [pltpu.VMEM(latents.shape, jnp.float32), pltpu.VMEM((latents.shape[0], 128), jnp.float32)],
        "partial",
    )(rank, latents, pixel_keys, pixel_values)
    pieces = [partials[0]] + [swap(partials[k], "pix", npix, k) for k in range(group - 1, 0, -1)]

    projected, = call(
        functools.partial(query_kernel, scale=scale), [pixel_queries.shape], [VMEM, VMEM], (), "queries"
    )(pixel_queries, w_key)

    for mask in outer:
        merged, = call(
            functools.partial(merge_kernel, rows=rows), [packed], [VMEM] * len(pieces), (), "merge"
        )(*pieces)
        pieces = [merged, swap(merged, "pix", npix, mask)]
    state, = call(
        functools.partial(state_kernel, rows=rows), [(rows, depth)], [SMEM, VMEM] + [VMEM] * len(pieces), (), "state"
    )(rank, latents, *pieces)
    states = [state] + [swap(state, "pix", npix, k) for k in range(1, group)]

    halves = min(2, nlat)
    half = lat & (halves - 1)
    ranks = jnp.stack([rank[0], half])
    qrows = pixel_queries.shape[0] // halves
    packed = (qrows + STAT, depth)
    reads = call(
        functools.partial(read_kernel, blocks=group, halves=halves),
        [latents.shape] + [packed] * halves,
        [SMEM, VMEM, VMEM] + [VMEM] * group,
        [pltpu.VMEM(pixel_queries.shape, jnp.float32), pltpu.VMEM((pixel_queries.shape[0], 128), jnp.float32)],
        "read",
    )(ranks, projected, norm_gain.reshape(1, depth), *states)
    latent_state, reads = reads[0], reads[1:]
    pieces = [reads[0]] + [swap(reads[k], "lat", nlat, k) for k in range(1, halves)]
    step = halves
    while step < nlat:
        merged, = call(
            functools.partial(merge_kernel, rows=qrows), [packed], [VMEM] * len(pieces), (), "merge"
        )(*pieces)
        pieces = [merged, swap(merged, "lat", nlat, step)]
        step *= 2
    mean, = call(
        functools.partial(mean_kernel, rows=qrows), [(qrows, depth)], [VMEM] * len(pieces), (), "mean"
    )(*pieces)
    means = [mean] + [swap(mean, "lat", nlat, k) for k in range(1, halves)]
    pixel_out, = call(
        functools.partial(out_kernel, halves=halves), [pixel_queries.shape], [SMEM, VMEM] + [VMEM] * halves, (), "out"
    )(half.reshape(1), w_value, *means)
    return latent_state, pixel_out


def solution(mesh):
    body = functools.partial(shards, npix=mesh.shape["pix"], nlat=mesh.shape["lat"])
    in_specs = (P("lat", None), P("pix", None), P("pix", None), P(), P(), P(), P("pix", None))
    out_specs = (P("lat", None), P("pix", None))
    return jax.shard_map(body, mesh=mesh, in_specs=in_specs, out_specs=out_specs, check_vma=False)
```

```python
import functools

import jax
import jax.numpy as jnp
from jax import lax
from jax.experimental import pallas as pl
from jax.experimental.pallas import tpu as pltpu
from jax.sharding import PartitionSpec as P


STAT = 8
CHUNKS = 2
F32, BF16 = jnp.float32, jnp.bfloat16
PARAMS = pltpu.CompilerParams(vmem_limit_bytes=24 * 1024 * 1024)
VMEM = pl.BlockSpec(memory_space=pltpu.VMEM)
SMEM = pl.BlockSpec(memory_space=pltpu.SMEM)
ANY = pl.BlockSpec(memory_space=pltpu.HBM)
NT = ((1,), (1,))
NN = ((1,), (0,))


def split(x):
    hi = x.astype(BF16)
    lo = (x - hi.astype(F32)).astype(BF16)
    return hi, lo


def dot3(a, b, dims):
    (ah, al), (bh, bl) = a, b
    dot = functools.partial(lax.dot_general, dimension_numbers=(dims, ((), ())), preferred_element_type=F32)
    return dot(ah, bh) + (dot(ah, bl) + dot(al, bh))


def call(body, outs, specs, scratch=(), out_specs=None):
    shapes = tuple(jax.ShapeDtypeStruct(*(s if isinstance(s[0], tuple) else (s, F32))) for s in outs)
    return pl.pallas_call(
        body,
        out_shape=shapes,
        in_specs=list(specs),
        out_specs=tuple(out_specs or [VMEM] * len(outs)),
        scratch_shapes=list(scratch),
        compiler_params=PARAMS,
    )


def pack_stats(top, total):
    rows = top.shape[0]
    lane = lax.broadcasted_iota(jnp.int32, (rows, 128), 1)
    wide = jnp.where(lane == 0, top, jnp.where(lane == 1, total, 0.0))
    return wide.T[:STAT]


def unpack_stats(tile):
    wide = jnp.concatenate([tile] * (128 // STAT), axis=0).T
    return wide[:, 0:1], wide[:, 1:2]


def attend(scores):
    top = jnp.max(scores, axis=1, keepdims=True)
    weights = jnp.exp(scores - top)
    return top, weights, jnp.sum(weights, axis=1, keepdims=True)


def merge(parts):
    top = functools.reduce(jnp.maximum, [p[0] for p in parts])
    total = weighted = None
    for t, s, w in parts:
        scale = jnp.exp(t - top)
        total = s * scale if total is None else total + s * scale
        weighted = w * scale if weighted is None else weighted + w * scale
    return top, total, weighted


def load_packed(ref, rows):
    top, total = unpack_stats(ref[rows:rows + STAT, :rows])
    return top, total, ref[:rows]


def store_packed(ref, rows, part):
    top, total, weighted = part
    ref[:rows] = weighted
    ref[rows:rows + STAT, :rows] = pack_stats(top, total)
    if rows < ref.shape[1]:
        ref[rows:rows + STAT, rows:] = jnp.zeros((STAT, ref.shape[1] - rows), F32)


def store_blocks(outs, part):
    top, total, weighted = part
    rows = top.shape[0] // len(outs)
    for k, out in enumerate(outs):
        at = slice(k * rows, (k + 1) * rows)
        store_packed(out, rows, (top[at], total[at], weighted[at]))


def partial_of(queries, keys, values, scale):
    top, weights, total = attend(dot3(split(queries * scale), keys, NT))
    return top, total, dot3(split(weights), values, NN)


def first_kernel(rank, latents, keys, values, *rest, blocks, scale):
    rest = list(rest)
    outs = [rest.pop(0) for _ in range(blocks)]
    chunks = [rest.pop(0) for _ in range(CHUNKS)]
    kh, kl, vh, vl, kbuf, vbuf, qsem, ksem, vsem = rest
    rows = chunks[0].shape[0] // blocks

    def query_copies(a):
        copies = []
        for k in range(blocks):
            at = pl.multiple_of((rank[0] ^ k) * (rows * CHUNKS) + a * rows, 8)
            copies.append(pltpu.make_async_copy(
                latents.at[pl.ds(at, rows), :], chunks[a].at[pl.ds(k * rows, rows), :], qsem.at[a, k]))
        return copies

    pieces = ksem.shape[0]
    size = kbuf.shape[0] // pieces

    def copies_of(src, dst, sem):
        return [pltpu.make_async_copy(src.at[pl.ds(i * size, size), :], dst.at[pl.ds(i * size, size), :], sem.at[i])
                for i in range(pieces)]

    queries = [query_copies(a) for a in range(CHUNKS)]
    key_copies, value_copies = copies_of(keys, kbuf, ksem), copies_of(values, vbuf, vsem)
    for copy in queries[0] + key_copies + value_copies + sum(queries[1:], []):
        copy.start()
    for copy in queries[0] + key_copies:
        copy.wait()
    kh[...], kl[...] = split(kbuf[...])
    top, weights, total = attend(dot3(split(chunks[0][...] * scale), (kh[...], kl[...]), NT))
    for copy in value_copies:
        copy.wait()
    vh[...], vl[...] = split(vbuf[...])
    store_blocks(outs, (top, total, dot3(split(weights), (vh[...], vl[...]), NN)))
    for copy in sum(queries[1:], []):
        copy.wait()


def partial_kernel(queries, kh, kl, vh, vl, *outs, scale):
    store_blocks(outs, partial_of(queries[...], (kh[...], kl[...]), (vh[...], vl[...]), scale))


def merge_kernel(*refs, rows):
    store_packed(refs[-1], rows, merge([load_packed(r, rows) for r in refs[:-1]]))


def state_kernel(latents, *refs, rows):
    _, total, weighted = merge([load_packed(r, rows) for r in refs[:-1]])
    refs[-1][...] = latents[:rows] + weighted / total


def query_kernel(half, queries, w_key, *outs, halves, scale):
    weight = split(w_key[...])
    rows = queries.shape[0] // halves // CHUNKS
    for b in range(CHUNKS):
        picked = []
        for k in range(halves):
            at = pl.multiple_of((half[0] ^ k) * (rows * CHUNKS) + b * rows, 8)
            picked.append(queries[pl.ds(at, rows), :])
        hi, lo = split(dot3(split(jnp.concatenate(picked, axis=0) * scale), weight, NT))
        outs[2 * b][...] = hi
        outs[2 * b + 1][...] = lo


def normed_of(states, gain):
    state = jnp.concatenate([s[...] for s in states], axis=0)
    return state / jnp.sqrt(jnp.mean(state * state, axis=1, keepdims=True) + 1e-06) * gain[...]


def early_kernel(gain, *refs, blocks):
    queries, states, outs = refs[:2 * CHUNKS], refs[2 * CHUNKS:2 * CHUNKS + blocks], refs[2 * CHUNKS + blocks:]
    normed = split(normed_of(states, gain))
    for b in range(CHUNKS):
        top, weights, total = attend(dot3((queries[2 * b][...], queries[2 * b + 1][...]), normed, NT))
        outs[2 * b][...] = dot3(split(weights), normed, NN)
        lane = lax.broadcasted_iota(jnp.int32, outs[2 * b + 1].shape, 1)
        outs[2 * b + 1][...] = jnp.where(lane == 0, top, total)


def late_kernel(gain, qh, ql, acc, stats, *refs, blocks, halves):
    states, outs = refs[:blocks], refs[blocks:]
    normed = split(normed_of(states, gain))
    scores = dot3((qh[...], ql[...]), normed, NT)
    before, before_total = stats[:, 0:1], stats[:, 1:2]
    top = jnp.maximum(before, jnp.max(scores, axis=1, keepdims=True))
    weights = jnp.exp(scores - top)
    keep = jnp.exp(before - top)
    total = before_total * keep + jnp.sum(weights, axis=1, keepdims=True)
    store_blocks(outs, (top, total, acc[...] * keep + dot3(split(weights), normed, NN)))


def mean_kernel(*refs, rows):
    _, total, weighted = merge([load_packed(r, rows) for r in refs[:-1]])
    refs[-1][...] = weighted / total


def mean_state_kernel(rank, *refs, rows, parts, blocks):
    pieces, states = refs[:parts], refs[parts:parts + blocks * CHUNKS]
    out, state_out, sems = refs[parts + blocks * CHUNKS:]
    size = states[0].shape[0]
    copies = []
    for a in range(CHUNKS):
        for k in range(blocks):
            at = pl.multiple_of((rank[0] ^ k) * (size * CHUNKS) + a * size, 8)
            copies.append(pltpu.make_async_copy(
                states[a * blocks + k], state_out.at[pl.ds(at, size), :], sems.at[a, k]))
    for copy in copies:
        copy.start()
    mean_kernel(*pieces, out, rows=rows)
    for copy in copies:
        copy.wait()


def project_kernel(w_value, *refs):
    weight = split(w_value[...])
    half = len(refs) // 2
    for src, dst in zip(refs[:half], refs[half:]):
        dst[...] = dot3(split(src[...]), weight, NN)


def out_kernel(half, w_value, *refs, halves):
    ready, last = refs[:halves * (CHUNKS - 1)], refs[halves * (CHUNKS - 1):halves * CHUNKS]
    out, buf, sems = refs[halves * CHUNKS:]
    rows = last[0].shape[0]

    def copy_out(src, b, k):
        at = pl.multiple_of((half[0] ^ k) * (rows * CHUNKS) + b * rows, 8)
        return pltpu.make_async_copy(src, out.at[pl.ds(at, rows), :], sems.at[b, k])

    copies = [copy_out(ready[b * halves + k], b, k) for b in range(CHUNKS - 1) for k in range(halves)]
    for copy in copies:
        copy.start()
    weight = split(w_value[...])
    for k in range(halves):
        buf[pl.ds(k * rows, rows), :] = dot3(split(last[k][...]), weight, NN)
        copies.append(copy_out(buf.at[pl.ds(k * rows, rows), :], CHUNKS - 1, k))
        copies[-1].start()
    for copy in copies:
        copy.wait()


def swap(value, axis, n, mask):
    return lax.ppermute(value, axis, [(i, i ^ mask) for i in range(n)])


def shards(latents, pixel_keys, pixel_values, norm_gain, w_key, w_value, pixel_queries, *, npix, nlat):
    return window(latents, pixel_keys, pixel_values, norm_gain, w_key, w_value, pixel_queries, npix, nlat)


def window(latents, pixel_keys, pixel_values, norm_gain, w_key, w_value, pixel_queries, npix, nlat):
    depth = latents.shape[1]
    scale = depth ** -0.5
    pix, lat = lax.axis_index("pix"), lax.axis_index("lat")
    group = min(4, npix)
    rank = pix & (group - 1)
    outer = []
    step = group
    while step < npix:
        outer.append(step)
        step *= 2
    if outer and group == 4:
        outer[0] = 6
        rank = rank ^ jnp.where(pix & 4, 2, 0)
    rank = rank.reshape(1)
    halves = min(2, nlat)
    half = (lat & (halves - 1)).reshape(1)

    rows = latents.shape[0] // group // CHUNKS
    packed = (rows + STAT, depth)
    chunk = (latents.shape[0] // CHUNKS, depth)
    keys_shape = pixel_keys.shape
    first = call(
        functools.partial(first_kernel, blocks=group, scale=scale),
        [packed] * group + [chunk] * CHUNKS + [(keys_shape, BF16)] * 4,
        [SMEM, ANY, ANY, ANY],
        [pltpu.VMEM(keys_shape, F32), pltpu.VMEM(keys_shape, F32), pltpu.SemaphoreType.DMA((CHUNKS, group)),
         pltpu.SemaphoreType.DMA((4,)), pltpu.SemaphoreType.DMA((4,))])(rank, *[pltpu.with_memory_space_constraint(x, pltpu.HBM) for x in (latents, pixel_keys, pixel_values)])
    latent_chunks = first[group:group + CHUNKS]
    operands = first[group + CHUNKS:]
    partials = [first[:group]]
    for a in range(1, CHUNKS):
        partials.append(call(
            functools.partial(partial_kernel, scale=scale), [packed] * group, [VMEM] * 5, ())(latent_chunks[a], *operands))

    pieces = [[part[0]] + [swap(part[k], "pix", npix, k) for k in range(group - 1, 0, -1)]
              for part in partials]
    queries = call(
        functools.partial(query_kernel, halves=halves, scale=scale),
        [((pixel_queries.shape[0] // CHUNKS, depth), BF16)] * (2 * CHUNKS),
        [SMEM, VMEM, VMEM], ())(half, pixel_queries, w_key)

    for mask in outer:
        for a in range(CHUNKS):
            merged, = call(
                functools.partial(merge_kernel, rows=rows), [packed], [VMEM] * len(pieces[a]), ())(*pieces[a])
            pieces[a] = [merged, swap(merged, "pix", npix, mask)]
    states = []
    for a in range(CHUNKS):
        state, = call(
            functools.partial(state_kernel, rows=rows), [(rows, depth)], [VMEM] * (1 + len(pieces[a])), ())(latent_chunks[a], *pieces[a])
        states.append([state] + [swap(state, "pix", npix, k) for k in range(1, group)])

    gain = norm_gain.reshape(1, depth)
    qchunk = pixel_queries.shape[0] // CHUNKS
    qrows = qchunk // halves
    early = call(
        functools.partial(early_kernel, blocks=group),
        [(qchunk, depth), (qchunk, 128)] * CHUNKS, [VMEM] * (1 + 2 * CHUNKS + group), ())(gain, *queries, *states[0])
    packed = (qrows + STAT, depth)
    pieces = []
    for b in range(CHUNKS):
        late = call(
            functools.partial(late_kernel, blocks=group, halves=halves),
            [packed] * halves, [VMEM] * (5 + group), ())(gain, queries[2 * b], queries[2 * b + 1], early[2 * b], early[2 * b + 1], *states[1])
        pieces.append([late[0]] + [swap(late[k], "lat", nlat, k) for k in range(1, halves)])
    step = halves
    while step < nlat:
        for b in range(CHUNKS):
            merged, = call(
                functools.partial(merge_kernel, rows=qrows), [packed], [VMEM] * len(pieces[b]), ())(*pieces[b])
            pieces[b] = [merged, swap(merged, "lat", nlat, step)]
        step *= 2
    means = []
    for b in range(CHUNKS):
        if b == 0:
            mean, latent_state = call(
                functools.partial(mean_state_kernel, rows=qrows, parts=len(pieces[b]), blocks=group),
                [(qrows, depth), latents.shape], [SMEM] + [VMEM] * (len(pieces[b]) + group * CHUNKS),
                [pltpu.SemaphoreType.DMA((CHUNKS, group))], [VMEM, ANY])(rank, *pieces[b], *sum(states, []))
        else:
            mean, = call(
                functools.partial(mean_kernel, rows=qrows), [(qrows, depth)], [VMEM] * len(pieces[b]), ())(*pieces[b])
        means.append([mean] + [swap(mean, "lat", nlat, k) for k in range(1, halves)])
    ready = []
    for b in range(CHUNKS - 1):
        ready += call(
            project_kernel, [(qrows, depth)] * halves, [VMEM] * (1 + halves), ())(w_value, *means[b])
    pixel_out, = call(
        functools.partial(out_kernel, halves=halves), [pixel_queries.shape],
        [SMEM, VMEM] + [VMEM] * (halves * CHUNKS),
        [pltpu.VMEM((halves * qrows, depth), F32), pltpu.SemaphoreType.DMA((CHUNKS, halves))],
        [ANY])(half, w_value, *ready, *means[-1])
    return latent_state, pixel_out


def solution(mesh):
    body = functools.partial(shards, npix=mesh.shape["pix"], nlat=mesh.shape["lat"])
    in_specs = (P("lat", None), P("pix", None), P("pix", None), P(), P(), P(), P("pix", None))
    out_specs = (P("lat", None), P("pix", None))
    return jax.shard_map(body, mesh=mesh, in_specs=in_specs, out_specs=out_specs, check_vma=False)
```

```python
import functools

import jax
import jax.numpy as jnp
from jax import lax
from jax.experimental import pallas as pl
from jax.experimental.pallas import tpu as pltpu
from jax.sharding import PartitionSpec as P


STAT = 8
CHUNKS = 2
F32, BF16 = jnp.float32, jnp.bfloat16
PARAMS = pltpu.CompilerParams(vmem_limit_bytes=16 * 1024 * 1024)
VMEM = pl.BlockSpec(memory_space=pltpu.VMEM)
SMEM = pl.BlockSpec(memory_space=pltpu.SMEM)
ANY = pl.BlockSpec(memory_space=pltpu.HBM)
NT = ((1,), (1,))
NN = ((1,), (0,))


def split(x):
    hi = x.astype(BF16)
    lo = (x - hi.astype(F32)).astype(BF16)
    return hi, lo


def dot3(a, b, dims):
    (ah, al), (bh, bl) = a, b
    dot = functools.partial(lax.dot_general, dimension_numbers=(dims, ((), ())), preferred_element_type=F32)
    return dot(ah, bh) + (dot(ah, bl) + dot(al, bh))


def call(body, outs, specs, scratch=(), out_specs=None):
    shapes = tuple(jax.ShapeDtypeStruct(*(s if isinstance(s[0], tuple) else (s, F32))) for s in outs)
    return pl.pallas_call(
        body,
        out_shape=shapes,
        in_specs=list(specs),
        out_specs=tuple(out_specs or [VMEM] * len(outs)),
        scratch_shapes=list(scratch),
        compiler_params=PARAMS,
    )


def pack_stats(top, total):
    rows = top.shape[0]
    lane = lax.broadcasted_iota(jnp.int32, (rows, 128), 1)
    wide = jnp.where(lane == 0, top, jnp.where(lane == 1, total, 0.0))
    return wide.T[:STAT]


def unpack_stats(tile):
    wide = jnp.concatenate([tile] * (128 // STAT), axis=0).T
    return wide[:, 0:1], wide[:, 1:2]


def attend(scores):
    top = jnp.max(scores, axis=1, keepdims=True)
    weights = jnp.exp(scores - top)
    return top, weights, jnp.sum(weights, axis=1, keepdims=True)


def merge(parts):
    top = functools.reduce(jnp.maximum, [p[0] for p in parts])
    total = weighted = None
    for t, s, w in parts:
        scale = jnp.exp(t - top)
        total = s * scale if total is None else total + s * scale
        weighted = w * scale if weighted is None else weighted + w * scale
    return top, total, weighted


def load_packed(ref, rows):
    top, total = unpack_stats(ref[rows:rows + STAT, :rows])
    return top, total, ref[:rows]


def store_packed(ref, rows, part):
    top, total, weighted = part
    ref[:rows] = weighted
    ref[rows:rows + STAT, :rows] = pack_stats(top, total)
    if rows < ref.shape[1]:
        ref[rows:rows + STAT, rows:] = jnp.zeros((STAT, ref.shape[1] - rows), F32)


def store_blocks(outs, part):
    top, total, weighted = part
    rows = top.shape[0] // len(outs)
    for k, out in enumerate(outs):
        at = slice(k * rows, (k + 1) * rows)
        store_packed(out, rows, (top[at], total[at], weighted[at]))


def partial_of(queries, keys, values, scale):
    top, weights, total = attend(dot3(split(queries * scale), keys, NT))
    return top, total, dot3(split(weights), values, NN)


def first_kernel(rank, latents, keys, values, *rest, blocks, scale):
    rest = list(rest)
    outs = [rest.pop(0) for _ in range(blocks)]
    chunks = [rest.pop(0) for _ in range(CHUNKS)]
    kh, kl, vh, vl, kbuf, vbuf, qsem, ksem, vsem = rest
    rows = chunks[0].shape[0] // blocks

    def query_copies(a):
        copies = []
        for k in range(blocks):
            at = pl.multiple_of((rank[0] ^ k) * (rows * CHUNKS) + a * rows, 8)
            copies.append(pltpu.make_async_copy(
                latents.at[pl.ds(at, rows), :], chunks[a].at[pl.ds(k * rows, rows), :], qsem.at[a, k]))
        return copies

    pieces = ksem.shape[0]
    size = kbuf.shape[0] // pieces

    def copies_of(src, dst, sem):
        return [pltpu.make_async_copy(src.at[pl.ds(i * size, size), :], dst.at[pl.ds(i * size, size), :], sem.at[i])
                for i in range(pieces)]

    queries = [query_copies(a) for a in range(CHUNKS)]
    key_copies, value_copies = copies_of(keys, kbuf, ksem), copies_of(values, vbuf, vsem)
    for copy in queries[0] + key_copies + value_copies + sum(queries[1:], []):
        copy.start()
    for copy in queries[0] + key_copies:
        copy.wait()
    kh[...], kl[...] = split(kbuf[...])
    top, weights, total = attend(dot3(split(chunks[0][...] * scale), (kh[...], kl[...]), NT))
    for copy in value_copies:
        copy.wait()
    vh[...], vl[...] = split(vbuf[...])
    store_blocks(outs, (top, total, dot3(split(weights), (vh[...], vl[...]), NN)))
    for copy in sum(queries[1:], []):
        copy.wait()


def partial_kernel(queries, kh, kl, vh, vl, *outs, scale):
    store_blocks(outs, partial_of(queries[...], (kh[...], kl[...]), (vh[...], vl[...]), scale))


def merge_kernel(*refs, rows):
    store_packed(refs[-1], rows, merge([load_packed(r, rows) for r in refs[:-1]]))


def state_kernel(latents, *refs, rows):
    _, total, weighted = merge([load_packed(r, rows) for r in refs[:-1]])
    refs[-1][...] = latents[:rows] + weighted / total


def query_kernel(half, queries, w_key, gain, *rest, halves, scale):
    outs, (buf, wbuf, sems) = rest[:2 * CHUNKS + 1], rest[2 * CHUNKS + 1:]
    rows = queries.shape[0] // halves // CHUNKS
    copies = [pltpu.make_async_copy(w_key, wbuf, sems.at[CHUNKS, 0]), pltpu.make_async_copy(gain, outs[-1], sems.at[CHUNKS, 1])]
    for b in range(CHUNKS):
        for k in range(halves):
            at = pl.multiple_of((half[0] ^ k) * (rows * CHUNKS) + b * rows, 8)
            copies.append(pltpu.make_async_copy(
                queries.at[pl.ds(at, rows), :], buf.at[pl.ds((b * halves + k) * rows, rows), :], sems.at[b, k]))
    for copy in copies:
        copy.start()
    for copy in copies:
        copy.wait()
    weight = split(wbuf[...])
    for b in range(CHUNKS):
        at = pl.ds(b * halves * rows, halves * rows)
        outs[2 * b][...], outs[2 * b + 1][...] = split(dot3(split(buf[at, :] * scale), weight, NT))


def normed_of(states, gain):
    state = jnp.concatenate([s[...] for s in states], axis=0)
    return state / jnp.sqrt(jnp.mean(state * state, axis=1, keepdims=True) + 1e-06) * gain[...]


def early_kernel(gain, *refs, blocks):
    queries, states, outs = refs[:2 * CHUNKS], refs[2 * CHUNKS:2 * CHUNKS + blocks], refs[2 * CHUNKS + blocks:]
    normed = split(normed_of(states, gain))
    for b in range(CHUNKS):
        top, weights, total = attend(dot3((queries[2 * b][...], queries[2 * b + 1][...]), normed, NT))
        outs[2 * b][...] = dot3(split(weights), normed, NN)
        lane = lax.broadcasted_iota(jnp.int32, outs[2 * b + 1].shape, 1)
        outs[2 * b + 1][...] = jnp.where(lane == 0, top, total)


def late_kernel(gain, qh, ql, acc, stats, *refs, blocks, halves):
    states, outs = refs[:blocks], refs[blocks:]
    normed = split(normed_of(states, gain))
    scores = dot3((qh[...], ql[...]), normed, NT)
    before, before_total = stats[:, 0:1], stats[:, 1:2]
    top = jnp.maximum(before, jnp.max(scores, axis=1, keepdims=True))
    weights = jnp.exp(scores - top)
    keep = jnp.exp(before - top)
    total = before_total * keep + jnp.sum(weights, axis=1, keepdims=True)
    store_blocks(outs, (top, total, acc[...] * keep + dot3(split(weights), normed, NN)))


def mean_kernel(*refs, rows):
    _, total, weighted = merge([load_packed(r, rows) for r in refs[:-1]])
    refs[-1][...] = weighted / total


def mean_state_kernel(rank, *refs, rows, parts, blocks):
    pieces, states = refs[:parts], refs[parts:parts + blocks * CHUNKS]
    out, state_out, sems = refs[parts + blocks * CHUNKS:]
    size = states[0].shape[0]
    copies = []
    for a in range(CHUNKS):
        for k in range(blocks):
            at = pl.multiple_of((rank[0] ^ k) * (size * CHUNKS) + a * size, 8)
            copies.append(pltpu.make_async_copy(
                states[a * blocks + k], state_out.at[pl.ds(at, size), :], sems.at[a, k]))
    for copy in copies:
        copy.start()
    mean_kernel(*pieces, out, rows=rows)
    for copy in copies:
        copy.wait()


def project_kernel(w_value, *refs):
    weight = split(w_value[...])
    half = len(refs) // 2
    for src, dst in zip(refs[:half], refs[half:]):
        dst[...] = dot3(split(src[...]), weight, NN)


def out_kernel(half, w_value, *refs, halves):
    ready, last = refs[:halves * (CHUNKS - 1)], refs[halves * (CHUNKS - 1):halves * CHUNKS]
    out, buf, sems = refs[halves * CHUNKS:]
    rows = last[0].shape[0]

    def copy_out(src, b, k):
        at = pl.multiple_of((half[0] ^ k) * (rows * CHUNKS) + b * rows, 8)
        return pltpu.make_async_copy(src, out.at[pl.ds(at, rows), :], sems.at[b, k])

    copies = [copy_out(ready[b * halves + k], b, k) for b in range(CHUNKS - 1) for k in range(halves)]
    for copy in copies:
        copy.start()
    weight = split(w_value[...])
    for k in range(halves):
        buf[pl.ds(k * rows, rows), :] = dot3(split(last[k][...]), weight, NN)
        copies.append(copy_out(buf.at[pl.ds(k * rows, rows), :], CHUNKS - 1, k))
        copies[-1].start()
    for copy in copies:
        copy.wait()


def swap(value, axis, n, mask):
    return lax.ppermute(value, axis, [(i, i ^ mask) for i in range(n)])


def in_hbm(*arrays):
    return [pltpu.with_memory_space_constraint(x, pltpu.HBM) for x in arrays]


def shards(latents, pixel_keys, pixel_values, norm_gain, w_key, w_value, pixel_queries, *, npix, nlat):
    return window(latents, pixel_keys, pixel_values, norm_gain, w_key, w_value, pixel_queries, npix, nlat)


def window(latents, pixel_keys, pixel_values, norm_gain, w_key, w_value, pixel_queries, npix, nlat):
    depth = latents.shape[1]
    scale = depth ** -0.5
    pix, lat = lax.axis_index("pix"), lax.axis_index("lat")
    group = min(4, npix)
    rank = pix & (group - 1)
    outer = []
    step = group
    while step < npix:
        outer.append(step)
        step *= 2
    if outer and group == 4:
        outer[0] = 6
        rank = rank ^ jnp.where(pix & 4, 2, 0)
    rank = rank.reshape(1)
    halves = min(2, nlat)
    half = (lat & (halves - 1)).reshape(1)

    rows = latents.shape[0] // group // CHUNKS
    packed = (rows + STAT, depth)
    chunk = (latents.shape[0] // CHUNKS, depth)
    keys_shape = pixel_keys.shape
    first = call(
        functools.partial(first_kernel, blocks=group, scale=scale),
        [packed] * group + [chunk] * CHUNKS + [(keys_shape, BF16)] * 4,
        [SMEM, ANY, ANY, ANY],
        [pltpu.VMEM(keys_shape, F32), pltpu.VMEM(keys_shape, F32), pltpu.SemaphoreType.DMA((CHUNKS, group)),
         pltpu.SemaphoreType.DMA((4,)), pltpu.SemaphoreType.DMA((4,))])(rank, *in_hbm(latents, pixel_keys, pixel_values))
    latent_chunks = first[group:group + CHUNKS]
    operands = first[group + CHUNKS:]
    partials = [first[:group]]
    for a in range(1, CHUNKS):
        partials.append(call(
            functools.partial(partial_kernel, scale=scale), [packed] * group, [VMEM] * 5, ())(latent_chunks[a], *operands))

    pieces = [[part[0]] + [swap(part[k], "pix", npix, k) for k in range(1, group)]
              for part in partials]
    queries = call(
        functools.partial(query_kernel, halves=halves, scale=scale),
        [((pixel_queries.shape[0] // CHUNKS, depth), BF16)] * (2 * CHUNKS) + [(1, depth)],
        [SMEM, ANY, ANY, ANY],
        [pltpu.VMEM(pixel_queries.shape, F32), pltpu.VMEM(w_key.shape, F32), pltpu.SemaphoreType.DMA((CHUNKS + 1, 2))])(half, *in_hbm(pixel_queries, w_key, norm_gain.reshape(1, depth)))
    gain, queries = queries[-1], queries[:-1]

    for mask in outer:
        for a in range(CHUNKS):
            merged, = call(
                functools.partial(merge_kernel, rows=rows), [packed], [VMEM] * len(pieces[a]), ())(*pieces[a])
            pieces[a] = [merged, swap(merged, "pix", npix, mask)]
    states = []
    for a in range(CHUNKS):
        state, = call(
            functools.partial(state_kernel, rows=rows), [(rows, depth)], [VMEM] * (1 + len(pieces[a])), ())(latent_chunks[a], *pieces[a])
        states.append([state] + [swap(state, "pix", npix, k) for k in range(1, group)])

    qchunk = pixel_queries.shape[0] // CHUNKS
    qrows = qchunk // halves
    early = call(
        functools.partial(early_kernel, blocks=group),
        [(qchunk, depth), (qchunk, 128)] * CHUNKS, [VMEM] * (1 + 2 * CHUNKS + group), ())(gain, *queries, *states[0])
    packed = (qrows + STAT, depth)
    pieces = []
    for b in range(CHUNKS):
        late = call(
            functools.partial(late_kernel, blocks=group, halves=halves),
            [packed] * halves, [VMEM] * (5 + group), ())(gain, queries[2 * b], queries[2 * b + 1], early[2 * b], early[2 * b + 1], *states[1])
        pieces.append([late[0]] + [swap(late[k], "lat", nlat, k) for k in range(1, halves)])
    step = halves
    while step < nlat:
        for b in range(CHUNKS):
            merged, = call(
                functools.partial(merge_kernel, rows=qrows), [packed], [VMEM] * len(pieces[b]), ())(*pieces[b])
            pieces[b] = [merged, swap(merged, "lat", nlat, step)]
        step *= 2
    means = []
    for b in range(CHUNKS):
        if b == 0:
            mean, latent_state = call(
                functools.partial(mean_state_kernel, rows=qrows, parts=len(pieces[b]), blocks=group),
                [(qrows, depth), latents.shape], [SMEM] + [VMEM] * (len(pieces[b]) + group * CHUNKS),
                [pltpu.SemaphoreType.DMA((CHUNKS, group))], [VMEM, ANY])(rank, *pieces[b], *sum(states, []))
        else:
            mean, = call(
                functools.partial(mean_kernel, rows=qrows), [(qrows, depth)], [VMEM] * len(pieces[b]), ())(*pieces[b])
        means.append([mean] + [swap(mean, "lat", nlat, k) for k in range(1, halves)])
    ready = []
    for b in range(CHUNKS - 1):
        ready += call(
            project_kernel, [(qrows, depth)] * halves, [VMEM] * (1 + halves), ())(w_value, *means[b])
    pixel_out, = call(
        functools.partial(out_kernel, halves=halves), [pixel_queries.shape],
        [SMEM, VMEM] + [VMEM] * (halves * CHUNKS),
        [pltpu.VMEM((halves * qrows, depth), F32), pltpu.SemaphoreType.DMA((CHUNKS, halves))],
        [ANY])(half, w_value, *ready, *means[-1])
    return latent_state, pixel_out


def solution(mesh):
    body = functools.partial(shards, npix=mesh.shape["pix"], nlat=mesh.shape["lat"])
    in_specs = (P("lat", None), P("pix", None), P("pix", None), P(), P(), P(), P("pix", None))
    out_specs = (P("lat", None), P("pix", None))
    return jax.shard_map(body, mesh=mesh, in_specs=in_specs, out_specs=out_specs, check_vma=False)
```

```python
import functools

import jax
import jax.numpy as jnp
from jax import lax
from jax.experimental import pallas as pl
from jax.experimental.pallas import tpu as pltpu
from jax.sharding import PartitionSpec as P


STAT = 8
CHUNKS = 2
F32, BF16 = jnp.float32, jnp.bfloat16
PARAMS = pltpu.CompilerParams(vmem_limit_bytes=16 * 1024 * 1024)
VMEM = pl.BlockSpec(memory_space=pltpu.VMEM)
SMEM = pl.BlockSpec(memory_space=pltpu.SMEM)
ANY = pl.BlockSpec(memory_space=pltpu.HBM)
NT = ((1,), (1,))
NN = ((1,), (0,))


def split(x):
    hi = x.astype(BF16)
    lo = (x - hi.astype(F32)).astype(BF16)
    return hi, lo


def dot3(a, b, dims):
    (ah, al), (bh, bl) = a, b
    dot = functools.partial(lax.dot_general, dimension_numbers=(dims, ((), ())), preferred_element_type=F32)
    return dot(ah, bh) + (dot(ah, bl) + dot(al, bh))


def call(body, outs, specs, scratch=(), out_specs=None):
    shapes = tuple(jax.ShapeDtypeStruct(*(s if isinstance(s[0], tuple) else (s, F32))) for s in outs)
    return pl.pallas_call(
        body,
        out_shape=shapes,
        in_specs=list(specs),
        out_specs=tuple(out_specs or [VMEM] * len(outs)),
        scratch_shapes=list(scratch),
        compiler_params=PARAMS,
    )


def pack_stats(top, total):
    rows = top.shape[0]
    lane = lax.broadcasted_iota(jnp.int32, (rows, 128), 1)
    wide = jnp.where(lane == 0, top, jnp.where(lane == 1, total, 0.0))
    return wide.T[:STAT]


def unpack_stats(tile):
    wide = jnp.concatenate([tile] * (128 // STAT), axis=0).T
    return wide[:, 0:1], wide[:, 1:2]


def attend(scores):
    top = jnp.max(scores, axis=1, keepdims=True)
    weights = jnp.exp(scores - top)
    return top, weights, jnp.sum(weights, axis=1, keepdims=True)


def merge(parts):
    top = functools.reduce(jnp.maximum, [p[0] for p in parts])
    total = weighted = None
    for t, s, w in parts:
        scale = jnp.exp(t - top)
        total = s * scale if total is None else total + s * scale
        weighted = w * scale if weighted is None else weighted + w * scale
    return top, total, weighted


def load_packed(ref, rows):
    top, total = unpack_stats(ref[rows:rows + STAT, :rows])
    return top, total, ref[:rows]


def store_packed(ref, rows, part):
    top, total, weighted = part
    ref[:rows] = weighted
    ref[rows:rows + STAT, :rows] = pack_stats(top, total)
    if rows < ref.shape[1]:
        ref[rows:rows + STAT, rows:] = jnp.zeros((STAT, ref.shape[1] - rows), F32)


def store_blocks(outs, part):
    top, total, weighted = part
    rows = top.shape[0] // len(outs)
    for k, out in enumerate(outs):
        at = slice(k * rows, (k + 1) * rows)
        store_packed(out, rows, (top[at], total[at], weighted[at]))


def partial_of(queries, keys, values, scale):
    top, weights, total = attend(dot3(split(queries * scale), keys, NT))
    return top, total, dot3(split(weights), values, NN)


def first_kernel(rank, latents, keys, values, *rest, blocks, scale):
    rest = list(rest)
    outs = [rest.pop(0) for _ in range(blocks)]
    chunks = [rest.pop(0) for _ in range(CHUNKS)]
    kh, kl, vh, vl, kbuf, vbuf, qsem, ksem, vsem = rest
    rows = chunks[0].shape[0] // blocks

    def query_copies(a):
        copies = []
        for k in range(blocks):
            at = pl.multiple_of((rank[0] ^ k) * (rows * CHUNKS) + a * rows, 8)
            copies.append(pltpu.make_async_copy(
                latents.at[pl.ds(at, rows), :], chunks[a].at[pl.ds(k * rows, rows), :], qsem.at[a, k]))
        return copies

    pieces = ksem.shape[0]
    size = kbuf.shape[0] // pieces

    def copies_of(src, dst, sem):
        return [pltpu.make_async_copy(src.at[pl.ds(i * size, size), :], dst.at[pl.ds(i * size, size), :], sem.at[i])
                for i in range(pieces)]

    queries = [query_copies(a) for a in range(CHUNKS)]
    key_copies, value_copies = copies_of(keys, kbuf, ksem), copies_of(values, vbuf, vsem)
    for copy in queries[0] + key_copies + value_copies + sum(queries[1:], []):
        copy.start()
    for copy in queries[0] + key_copies:
        copy.wait()
    kh[...], kl[...] = split(kbuf[...])
    top, weights, total = attend(dot3(split(chunks[0][...] * scale), (kh[...], kl[...]), NT))
    for copy in value_copies:
        copy.wait()
    vh[...], vl[...] = split(vbuf[...])
    store_blocks(outs, (top, total, dot3(split(weights), (vh[...], vl[...]), NN)))
    for copy in sum(queries[1:], []):
        copy.wait()


def partial_kernel(queries, kh, kl, vh, vl, *outs, scale):
    store_blocks(outs, partial_of(queries[...], (kh[...], kl[...]), (vh[...], vl[...]), scale))


def merge_kernel(*refs, rows):
    store_packed(refs[-1], rows, merge([load_packed(r, rows) for r in refs[:-1]]))


def state_kernel(latents, *refs, rows):
    _, total, weighted = merge([load_packed(r, rows) for r in refs[:-1]])
    refs[-1][...] = latents[:rows] + weighted / total


def query_kernel(half, queries, w_key, gain, *rest, halves, scale):
    outs, (buf, wbuf, sems) = rest[:2 * CHUNKS + 1], rest[2 * CHUNKS + 1:]
    rows = queries.shape[0] // halves // CHUNKS
    copies = [pltpu.make_async_copy(w_key, wbuf, sems.at[CHUNKS, 0]), pltpu.make_async_copy(gain, outs[-1], sems.at[CHUNKS, 1])]
    for b in range(CHUNKS):
        for k in range(halves):
            at = pl.multiple_of((half[0] ^ k) * (rows * CHUNKS) + b * rows, 8)
            copies.append(pltpu.make_async_copy(
                queries.at[pl.ds(at, rows), :], buf.at[pl.ds((b * halves + k) * rows, rows), :], sems.at[b, k]))
    for copy in copies:
        copy.start()
    for copy in copies:
        copy.wait()
    weight = split(wbuf[...])
    for b in range(CHUNKS):
        at = pl.ds(b * halves * rows, halves * rows)
        outs[2 * b][...], outs[2 * b + 1][...] = split(dot3(split(buf[at, :] * scale), weight, NT))


def normed_of(states, gain):
    state = jnp.concatenate([s[...] for s in states], axis=0)
    return state / jnp.sqrt(jnp.mean(state * state, axis=1, keepdims=True) + 1e-06) * gain[...]


def early_kernel(gain, *refs, blocks):
    queries, states, outs = refs[:2 * CHUNKS], refs[2 * CHUNKS:2 * CHUNKS + blocks], refs[2 * CHUNKS + blocks:]
    normed = split(normed_of(states, gain))
    for b in range(CHUNKS):
        top, weights, total = attend(dot3((queries[2 * b][...], queries[2 * b + 1][...]), normed, NT))
        outs[2 * b][...] = dot3(split(weights), normed, NN)
        lane = lax.broadcasted_iota(jnp.int32, outs[2 * b + 1].shape, 1)
        outs[2 * b + 1][...] = jnp.where(lane == 0, top, total)


def late_kernel(gain, qh, ql, acc, stats, *refs, blocks, halves):
    states, outs = refs[:blocks], refs[blocks:]
    normed = split(normed_of(states, gain))
    scores = dot3((qh[...], ql[...]), normed, NT)
    before, before_total = stats[:, 0:1], stats[:, 1:2]
    top = jnp.maximum(before, jnp.max(scores, axis=1, keepdims=True))
    weights = jnp.exp(scores - top)
    keep = jnp.exp(before - top)
    total = before_total * keep + jnp.sum(weights, axis=1, keepdims=True)
    store_blocks(outs, (top, total, acc[...] * keep + dot3(split(weights), normed, NN)))


def mean_kernel(*refs, rows):
    _, total, weighted = merge([load_packed(r, rows) for r in refs[:-1]])
    refs[-1][...] = weighted / total


def mean_state_kernel(rank, *refs, rows, parts, blocks):
    pieces, states = refs[:parts], refs[parts:parts + blocks * CHUNKS]
    out, state_out, sems = refs[parts + blocks * CHUNKS:]
    size = states[0].shape[0]
    copies = []
    for a in range(CHUNKS):
        for k in range(blocks):
            at = pl.multiple_of((rank[0] ^ k) * (size * CHUNKS) + a * size, 8)
            copies.append(pltpu.make_async_copy(
                states[a * blocks + k], state_out.at[pl.ds(at, size), :], sems.at[a, k]))
    for copy in copies:
        copy.start()
    mean_kernel(*pieces, out, rows=rows)
    for copy in copies:
        copy.wait()


def project_kernel(w_value, *refs):
    *refs, hi_out, lo_out = refs
    hi_out[...], lo_out[...] = split(w_value[...])
    half = len(refs) // 2
    for src, dst in zip(refs[:half], refs[half:]):
        dst[...] = dot3(split(src[...]), (hi_out[...], lo_out[...]), NN)


def own_kernel(hi, lo, src, dst):
    dst[...] = dot3(split(src[...]), (hi[...], lo[...]), NN)


def out_kernel(half, hi, lo, *refs, halves):
    count = halves * CHUNKS
    ready, last = refs[:count - halves + 1], refs[count - halves + 1:count]
    out, buf, sems = refs[count:]
    rows = ready[0].shape[0]

    def copy_out(src, i):
        b, k = divmod(i, halves)
        at = pl.multiple_of((half[0] ^ k) * (rows * CHUNKS) + b * rows, 8)
        return pltpu.make_async_copy(src, out.at[pl.ds(at, rows), :], sems.at[b, k])

    copies = [copy_out(src, i) for i, src in enumerate(ready)]
    for copy in copies:
        copy.start()
    for i, src in enumerate(last):
        at = pl.ds(i * rows, rows)
        buf[at, :] = dot3(split(src[...]), (hi[...], lo[...]), NN)
        copies.append(copy_out(buf.at[at, :], len(ready) + i))
        copies[-1].start()
    for copy in copies:
        copy.wait()


def swap(value, axis, n, mask):
    return lax.ppermute(value, axis, [(i, i ^ mask) for i in range(n)])


def in_hbm(*arrays):
    return [pltpu.with_memory_space_constraint(x, pltpu.HBM) for x in arrays]


def shards(latents, pixel_keys, pixel_values, norm_gain, w_key, w_value, pixel_queries, *, npix, nlat):
    return window(latents, pixel_keys, pixel_values, norm_gain, w_key, w_value, pixel_queries, npix, nlat)


def window(latents, pixel_keys, pixel_values, norm_gain, w_key, w_value, pixel_queries, npix, nlat):
    depth = latents.shape[1]
    scale = depth ** -0.5
    pix, lat = lax.axis_index("pix"), lax.axis_index("lat")
    group = min(4, npix)
    rank = pix & (group - 1)
    outer = []
    step = group
    while step < npix:
        outer.append(step)
        step *= 2
    if outer and group == 4:
        outer[0] = 6
        rank = rank ^ jnp.where(pix & 4, 2, 0)
    rank = rank.reshape(1)
    halves = min(2, nlat)
    half = (lat & (halves - 1)).reshape(1)

    rows = latents.shape[0] // group // CHUNKS
    packed = (rows + STAT, depth)
    chunk = (latents.shape[0] // CHUNKS, depth)
    keys_shape = pixel_keys.shape
    first = call(
        functools.partial(first_kernel, blocks=group, scale=scale),
        [packed] * group + [chunk] * CHUNKS + [(keys_shape, BF16)] * 4,
        [SMEM, ANY, ANY, ANY],
        [pltpu.VMEM(keys_shape, F32), pltpu.VMEM(keys_shape, F32), pltpu.SemaphoreType.DMA((CHUNKS, group)),
         pltpu.SemaphoreType.DMA((4,)), pltpu.SemaphoreType.DMA((4,))])(rank, *in_hbm(latents, pixel_keys, pixel_values))
    latent_chunks = first[group:group + CHUNKS]
    operands = first[group + CHUNKS:]
    partials = [first[:group]]
    for a in range(1, CHUNKS):
        partials.append(call(
            functools.partial(partial_kernel, scale=scale), [packed] * group, [VMEM] * 5, ())(latent_chunks[a], *operands))

    pieces = [[part[0]] + [swap(part[k], "pix", npix, k) for k in range(1, group)]
              for part in partials]
    queries = call(
        functools.partial(query_kernel, halves=halves, scale=scale),
        [((pixel_queries.shape[0] // CHUNKS, depth), BF16)] * (2 * CHUNKS) + [(1, depth)],
        [SMEM, ANY, ANY, ANY],
        [pltpu.VMEM(pixel_queries.shape, F32), pltpu.VMEM(w_key.shape, F32), pltpu.SemaphoreType.DMA((CHUNKS + 1, 2))])(half, *in_hbm(pixel_queries, w_key, norm_gain.reshape(1, depth)))
    gain, queries = queries[-1], queries[:-1]

    for mask in outer:
        for a in range(CHUNKS):
            merged, = call(
                functools.partial(merge_kernel, rows=rows), [packed], [VMEM] * len(pieces[a]), ())(*pieces[a])
            pieces[a] = [merged, swap(merged, "pix", npix, mask)]
    states = []
    for a in range(CHUNKS):
        state, = call(
            functools.partial(state_kernel, rows=rows), [(rows, depth)], [VMEM] * (1 + len(pieces[a])), ())(latent_chunks[a], *pieces[a])
        states.append([state] + [swap(state, "pix", npix, k) for k in range(1, group)])

    qchunk = pixel_queries.shape[0] // CHUNKS
    qrows = qchunk // halves
    early = call(
        functools.partial(early_kernel, blocks=group),
        [(qchunk, depth), (qchunk, 128)] * CHUNKS, [VMEM] * (1 + 2 * CHUNKS + group), ())(gain, *queries, *states[0])
    packed = (qrows + STAT, depth)
    pieces = []
    for b in range(CHUNKS):
        late = call(
            functools.partial(late_kernel, blocks=group, halves=halves),
            [packed] * halves, [VMEM] * (5 + group), ())(gain, queries[2 * b], queries[2 * b + 1], early[2 * b], early[2 * b + 1], *states[1])
        pieces.append([late[0]] + [swap(late[k], "lat", nlat, k) for k in range(1, halves)])
    step = halves
    while step < nlat:
        for b in range(CHUNKS):
            merged, = call(
                functools.partial(merge_kernel, rows=qrows), [packed], [VMEM] * len(pieces[b]), ())(*pieces[b])
            pieces[b] = [merged, swap(merged, "lat", nlat, step)]
        step *= 2
    means = []
    for b in range(CHUNKS):
        if b == 0:
            mean, latent_state = call(
                functools.partial(mean_state_kernel, rows=qrows, parts=len(pieces[b]), blocks=group),
                [(qrows, depth), latents.shape], [SMEM] + [VMEM] * (len(pieces[b]) + group * CHUNKS),
                [pltpu.SemaphoreType.DMA((CHUNKS, group))], [VMEM, ANY])(rank, *pieces[b], *sum(states, []))
        else:
            mean, = call(
                functools.partial(mean_kernel, rows=qrows), [(qrows, depth)], [VMEM] * len(pieces[b]), ())(*pieces[b])
        means.append([mean] + [swap(mean, "lat", nlat, k) for k in range(1, halves)])
    ready = []
    for b in range(CHUNKS - 1):
        *done, hi, lo = call(
            project_kernel, [(qrows, depth)] * halves + [(w_value.shape, BF16)] * 2,
            [VMEM] * (1 + halves), ())(w_value, *means[b])
        ready += done
    own, = call(own_kernel, [(qrows, depth)], [VMEM] * 3, ())(hi, lo, means[-1][0])
    pixel_out, = call(
        functools.partial(out_kernel, halves=halves), [pixel_queries.shape],
        [SMEM] + [VMEM] * (2 + halves * CHUNKS),
        [pltpu.VMEM((max(halves - 1, 1) * qrows, depth), F32), pltpu.SemaphoreType.DMA((CHUNKS, halves))],
        [ANY])(half, hi, lo, *ready, own, *means[-1][1:])
    return latent_state, pixel_out


def solution(mesh):
    body = functools.partial(shards, npix=mesh.shape["pix"], nlat=mesh.shape["lat"])
    in_specs = (P("lat", None), P("pix", None), P("pix", None), P(), P(), P(), P("pix", None))
    out_specs = (P("lat", None), P("pix", None))
    return jax.shard_map(body, mesh=mesh, in_specs=in_specs, out_specs=out_specs, check_vma=False)
```
